32 devices in a mesh: gx: 8 (over z, x), gy: 4 (over y, core).
Axes of the slice: x: 2, y: 2, z: 4, core: 2. Of those that a mesh axis runs over, the one named last changes fastest.
Arguments:
- pressure: float32 [10, 512, 2048], P(None, 'gx', 'gy'), may hold values from -6 to 6
- pressure_old: float32 [10, 512, 2048], P(None, 'gx', 'gy'), may hold values from -6 to 6
- conductivity: float32 [10, 512, 2048], P(None, 'gx', 'gy'), may hold values from 0.1 to 1
- porosity: float32 [10, 512, 2048], P(None, 'gx', 'gy'), may hold values from 2 to 8
- recharge: float32 [512, 2048], P('gx', 'gy'), may hold values from -6 to 6
- active: int32 [512, 2048], P('gx', 'gy'), may hold values from 0 to 1, as said below
Outputs:
- final_pressure: float32 [10, 512, 2048], P(None, 'gx', 'gy')
- linear_residual: float32 [10, 512, 2048], P(None, 'gx', 'gy')
The draws below stay inside these ranges and needn't reach their ends.
Inputs may be any that keep to these rules, and one draw needn't show every extreme that they name: `active`: 1 marks a land column, 0 an ocean column.
All inputs are finite; a program needn't handle non-finite values.
Results may differ from the reference program's by a relative error of at most 0.0003.
Values sent between devices are 32-bit elements; how exact they have to be, the bound alone decides.
A program may use at most 128 MiB of HBM per device.

```python
import math
import jax
import jax.numpy as jnp

CX = 64
CY = 512
NZ = 10
STEPS = 1
NEWTON = 2
NX = 512
NY = 2048


def draw_active(key, part):
    key_corner = jax.random.fold_in(key, 11)
    key_jitter = jax.random.fold_in(key, 12)
    tiles_x = NX // CX
    tiles_y = NY // CY
    corners = jax.random.randint(key_corner, (tiles_x + 1, tiles_y + 1), 0, 10, dtype=jnp.int32)
    row_index = jnp.arange(NX, dtype=jnp.int32)
    row_tile = row_index // CX
    row_frac = row_index % CX
    blended = corners[row_tile] * (CX - row_frac)[:, None] + corners[row_tile + 1] * row_frac[:, None]
    column_index = jnp.arange(NY, dtype=jnp.int32)
    column_tile = column_index // CY
    column_frac = column_index % CY
    surface = blended[:, column_tile] * (CY - column_frac)[None] + blended[:, column_tile + 1] * column_frac[None]
    jitter = jax.random.randint(key_jitter, (NX, NY), 0, 3 * CX * CY, dtype=jnp.int32)
    land_mask = jnp.where(surface + jitter > 6 * CX * CY, 1, 0).astype(jnp.int32)
    land_mask = land_mask.at[0, 0].set(1)
    land_mask = land_mask.at[0, 1].set(0)
    return land_mask


def levels(rng, shape, pieces, least, top_value):
    gain, own = 1.0, jax.random.fold_in(rng, 6)
    for axis_at, parts in pieces:
        steps = jnp.exp(jax.random.uniform(jax.random.fold_in(own, axis_at), (parts,), jnp.float32, least / len(pieces), top_value / len(pieces)))
        gain = gain * jnp.repeat(steps, shape[axis_at] // parts).reshape([-1 if axis == axis_at else 1 for axis in range(len(shape))])
    return gain


def normal_values(stream_key, extent, deviation, most, pieces=(), kind=jnp.bfloat16):
    gain = levels(stream_key, extent, pieces, -0.22, 0.18) if pieces else 1.0
    result = jax.random.normal(stream_key, extent, jnp.float32) * deviation * gain
    return jnp.minimum(jnp.maximum(result, -most), most).astype(kind)


def setup_inputs(seed: int = 0) -> dict:
    streams_of = jax.random.split(jax.random.key(seed), 7)
    pressure = normal_values(streams_of[0], (NZ, NX, NY), 1.0, 6.0, ((1, 8), (2, 4)), jnp.float32)
    pressure_old = normal_values(streams_of[1], (NZ, NX, NY), 1.0, 6.0, ((1, 8), (2, 4)), jnp.float32)
    conductivity = jnp.clip(jnp.exp(math.log(1.0) - 2.3025851 * jax.random.uniform(streams_of[2], (NZ, NX, NY), jnp.float32) ** levels(streams_of[2], (NZ, NX, NY), ((1, 8), (2, 4)), -0.2, 0.2)), 0.1, 1.0)
    porosity = jnp.clip(jnp.exp(math.log(8.0) - 1.3862944 * jax.random.uniform(streams_of[3], (NZ, NX, NY), jnp.float32) ** levels(streams_of[3], (NZ, NX, NY), ((1, 8), (2, 4)), -0.2, 0.2)), 2.0, 8.0)
    recharge = normal_values(streams_of[4], (NX, NY), 1.0, 6.0, ((0, 8), (1, 4)), jnp.float32)
    active = draw_active(jax.random.fold_in(streams_of[6], 71), 0)
    return dict(pressure=pressure, pressure_old=pressure_old, conductivity=conductivity, porosity=porosity, recharge=recharge, active=active)


residual_sat = 0.1
vertical_factor = 2.0
epsilon = 1e-06

def interior(array):
    return array[:, 1:-1, 1:-1]

def saturation(values):
    return residual_sat + (1.0 - residual_sat) * jax.nn.sigmoid(values)

def sat_slope(values):
    sigma = jax.nn.sigmoid(values)
    return (1.0 - residual_sat) * sigma * (1.0 - sigma)

def face_pair(press_low, press_high, cond_low, cond_high, act_low, act_high, factor, gravity):
    transmit = 0.5 * factor * (cond_low + cond_high) * act_low * act_high
    sig_low = jax.nn.sigmoid(press_low)
    sig_high = jax.nn.sigmoid(press_high)
    mobility = 0.5 * (sig_low * sig_low + sig_high * sig_high)
    head_drop = press_low - press_high + gravity
    coef_low = transmit * (mobility + sig_low * sig_low * (1.0 - sig_low) * head_drop)
    coef_high = transmit * (sig_high * sig_high * (1.0 - sig_high) * head_drop - mobility)
    return (coef_low, coef_high, transmit * mobility * head_drop)

def coefficients(pressure, conduct, active):
    across_x = face_pair(pressure[:, :-1, 1:-1], pressure[:, 1:, 1:-1], conduct[:, :-1, 1:-1], conduct[:, 1:, 1:-1], active[:, :-1, 1:-1], active[:, 1:, 1:-1], 1.0, 0.0)
    across_y = face_pair(pressure[:, 1:-1, :-1], pressure[:, 1:-1, 1:], conduct[:, 1:-1, :-1], conduct[:, 1:-1, 1:], active[:, 1:-1, :-1], active[:, 1:-1, 1:], 1.0, 0.0)
    inner_p = interior(pressure)
    inner_k = interior(conduct)
    inner_a = interior(active)
    across_z = face_pair(inner_p[:-1], inner_p[1:], inner_k[:-1], inner_k[1:], inner_a[:-1], inner_a[1:], vertical_factor, -1.0)
    return (across_x, across_y, across_z)

def outflow(flow_x, flow_y, flow_z):
    total = flow_x[:, 1:] - flow_x[:, :-1] + flow_y[:, :, 1:] - flow_y[:, :, :-1]
    zeros = jnp.zeros_like(flow_z[:1])
    return total + jnp.concatenate([flow_z, zeros], 0) - jnp.concatenate([zeros, flow_z], 0)

def jacobian_apply(vector, faces, diagonal, active):
    x_low, x_high, x_flow = faces[0]
    y_low, y_high, y_flow = faces[1]
    z_low, z_high, z_flow = faces[2]
    flow_x = x_low * vector[:, :-1, 1:-1] + x_high * vector[:, 1:, 1:-1]
    flow_y = y_low * vector[:, 1:-1, :-1] + y_high * vector[:, 1:-1, 1:]
    center = interior(vector)
    flow_z = z_low * center[:-1] + z_high * center[1:]
    return active * (diagonal * center + outflow(flow_x, flow_y, flow_z)) + (1.0 - active) * center

def newton_residual(pressure, faces, pressure_old, porosity, recharge, active):
    center = interior(pressure)
    storage = porosity * (saturation(center) - saturation(pressure_old))
    inflow = jnp.concatenate([jnp.zeros_like(center[:-1]), recharge[None]], 0)
    flows = outflow(faces[0][2], faces[1][2], faces[2][2])
    return active * (storage - inflow + flows) + (1.0 - active) * center

def least_squares(first_norm, entry_one, entry_two, entry_three, entry_four, entry_five):
    radius = jnp.sqrt(entry_one * entry_one + entry_two * entry_two)
    cosine = entry_one / radius
    sine = entry_two / radius
    top_right = cosine * entry_three + sine * entry_four
    lower = cosine * entry_four - sine * entry_three
    weight_two = -lower * sine * first_norm / (lower * lower + entry_five * entry_five)
    weight_one = (cosine * first_norm - top_right * weight_two) / radius
    return (weight_one, weight_two)

def widen(array):
    return jnp.pad(array, ((0, 0), (1, 1), (1, 1)))

def reference(pressure, pressure_old, conductivity, porosity, recharge, active):
    active_cells = jnp.broadcast_to(active.astype(jnp.float32)[None], pressure.shape)
    cond_ext = widen(conductivity)
    active_ext = widen(active_cells)
    current = pressure
    previous = pressure_old
    leftover = jnp.zeros_like(pressure)
    for step_index in range(STEPS):
        for newton_index in range(NEWTON):
            current_ext = widen(current)
            faces = coefficients(current_ext, cond_ext, active_ext)
            remainder = -newton_residual(current_ext, faces, previous, porosity, recharge, active_cells)
            diagonal = porosity * sat_slope(current)
            first_norm = jnp.sqrt(jnp.sum(remainder * remainder) + epsilon)
            basis_one = remainder / first_norm
            image_one = jacobian_apply(widen(basis_one), faces, diagonal, active_cells)
            entry_one = jnp.sum(image_one * basis_one)
            ortho_one = image_one - entry_one * basis_one
            entry_two = jnp.sqrt(jnp.sum(ortho_one * ortho_one) + epsilon)
            basis_two = ortho_one / entry_two
            image_two = jacobian_apply(widen(basis_two), faces, diagonal, active_cells)
            entry_three = jnp.sum(image_two * basis_one)
            entry_four = jnp.sum(image_two * basis_two)
            ortho_two = image_two - entry_three * basis_one - entry_four * basis_two
            entry_five = jnp.sqrt(jnp.sum(ortho_two * ortho_two) + epsilon)
            weight_one, weight_two = least_squares(first_norm, entry_one, entry_two, entry_three, entry_four, entry_five)
            current = current + (weight_one * basis_one + weight_two * basis_two)
            leftover = remainder - weight_one * image_one - weight_two * image_two
        previous = current
    return (current, leftover)
```

```python
import functools

import jax
import jax.numpy as jnp
from jax import lax
from jax.experimental import pallas as pl
from jax.experimental.pallas import tpu as pltpu
from jax.sharding import PartitionSpec as P

NEWTON = 2
residual_sat = 0.1
vertical_factor = 2.0
epsilon = 1e-06
T = 8
W = 128
MESH = pl.DeviceIdType.MESH


def sigmoid(v):
    return 1.0 / (1.0 + jnp.exp(jnp.minimum(-v, 87.0)))


def fold(v):
    out = v[:, :W]
    for j in range(1, v.shape[1] // W):
        out = out + v[:, j * W:(j + 1) * W]
    return out


def kernel(
    L, NX, NY, GX, GY,
    p_in, po_in, k_in, por_in, rech_in, act_in,
    p_out, l_out,
    pre, sre, are, bre, cre, acte, p9, r0,
    txp, txm, typ, tym, tzp,
    dg, oxp, oxm, oyp, oym, ozp, ozm,
    srow, scol, rrow, rcol, sumy, sumx,
    send_sem, recv_sem, ysend, yrecv, xsend, xrecv,
):
    R = NX // T
    gx = lax.axis_index("gx")
    gy = lax.axis_index("gy")
    f32 = jnp.float32
    row8 = lax.broadcasted_iota(jnp.int32, (T, NY), 0)
    lane = lax.broadcasted_iota(jnp.int32, (T, NY), 1)
    lane1 = lax.broadcasted_iota(jnp.int32, (T, W), 1)
    has = (gx > 0, gx < GX - 1, gy > 0, gy < GY - 1)

    rrow[...] = jnp.zeros_like(rrow)
    rcol[...] = jnp.zeros_like(rcol)

    barrier = pltpu.get_barrier_semaphore()
    for d in range(1, GX):
        pl.semaphore_signal(barrier, inc=1, device_id=(lax.rem(gx + d, GX), gy), device_id_type=MESH)
    for d in range(1, GY):
        pl.semaphore_signal(barrier, inc=1, device_id=(gx, lax.rem(gy + d, GY)), device_id_type=MESH)

    def tile(ref, k, r):
        return ref[k, pl.ds(pl.multiple_of((r + 1) * T, T), T), :]

    def plain(ref, k, r):
        return ref[k, pl.ds(pl.multiple_of(r * T, T), T), :]

    def put(ref, k, r, v):
        ref[k, pl.ds(pl.multiple_of(r * T, T), T), :] = v

    def up(ref, k, r, cur):
        return pltpu.roll(jnp.where(row8 == T - 1, tile(ref, k, r - 1), cur), 1, 0)

    def down(ref, k, r, cur):
        return pltpu.roll(jnp.where(row8 == 0, tile(ref, k, r + 1), cur), T - 1, 0)

    def wide(v):
        return jnp.concatenate([v] * (NY // W), axis=1)

    def left(cur, halo, k, r):
        h = pltpu.roll(halo, lax.rem(2 * W - (k * R + r), W), 1)
        return jnp.where(lane == 0, wide(h), pltpu.roll(cur, 1, 1))

    def right(cur, halo, k, r):
        h = pltpu.roll(halo, W - 1 - (k * R + r), 1)
        return jnp.where(lane == NY - 1, wide(h), pltpu.roll(cur, NY - 1, 1))

    def pack(acc, v, k, r):
        lo, hi = acc
        at = lane1 == k * R + r
        lo = jnp.where(at, jnp.broadcast_to(v[:, 0:1], (T, W)), lo)
        hi = jnp.where(at, jnp.broadcast_to(v[:, NY - 1:NY], (T, W)), hi)
        return lo, hi

    zero1 = jnp.zeros((T, W), f32)

    def copies(st, nr, nc):
        peers = ((gx - 1, gy), (gx + 1, gy), (gx, gy - 1), (gx, gy + 1))
        out = []
        for d in range(4):
            back = d ^ 1
            if d < 2:
                src, dst = srow.at[st, d, pl.ds(0, nr)], rrow.at[st, back, pl.ds(0, nr)]
            else:
                src, dst = scol.at[st, d - 2, pl.ds(0, nc)], rcol.at[st, back - 2, pl.ds(0, nc)]
            out.append((has[d], pltpu.make_async_remote_copy(
                src_ref=src, dst_ref=dst,
                send_sem=send_sem.at[st, d], recv_sem=recv_sem.at[st, back],
                device_id=peers[d], device_id_type=MESH)))
        return out

    def start(st, nr, nc):
        for cond, c in copies(st, nr, nc):
            @pl.when(cond)
            def _(c=c):
                c.start()

    def finish(st, nr, nc):
        for d, (cond, c) in enumerate(copies(st, nr, nc)):
            @pl.when(cond)
            def _(c=c):
                c.wait_send()
        cs = copies(st, nr, nc)
        for d in range(4):
            @pl.when(has[d])
            def _(d=d):
                cs[d ^ 1][1].wait_recv()

    NR0 = srow.shape[2]
    NRL = ((L + T - 1) // T) * T

    for e, row in ((0, 0), (1, NX - 1)):
        for k in range(L):
            srow[0, e, k:k + 1, :] = p_in[k, row:row + 1, :]
            srow[0, e, L + k:L + k + 1, :] = k_in[k, row:row + 1, :]
        srow[0, e, 2 * L:2 * L + 1, :] = act_in[row:row + 1, :].astype(f32)

    def pack0(r, c):
        pp, kk, aa = c
        for k in range(L):
            pp = pack(pp, plain(p_in, k, r), k, r)
            kk = pack(kk, plain(k_in, k, r), k, r)
        aa = pack(aa, act_in[pl.ds(pl.multiple_of(r * T, T), T), :].astype(f32), 0, r)
        return pp, kk, aa

    z2 = (zero1, zero1)
    pp, kk, aa = lax.fori_loop(0, R, pack0, (z2, z2, z2))
    for e in range(2):
        scol[0, e, 0:T, :] = pp[e]
        scol[0, e, T:2 * T, :] = kk[e]
        scol[0, e, 2 * T:3 * T, :] = aa[e]
    pl.semaphore_wait(barrier, GX - 1 + GY - 1)
    start(0, NR0, 3 * T)

    def local(r, c):
        act = act_in[pl.ds(pl.multiple_of(r * T, T), T), :].astype(f32)
        put(acte, 0, r + 1, act)
        for k in range(L):
            p = plain(p_in, k, r)
            put(pre, k, r + 1, p)
            put(sre, k, r + 1, sigmoid(p))
            put(are, k, r + 1, plain(k_in, k, r))
            w = (1.0 - residual_sat) * act * plain(por_in, k, r)
            put(p9, k, r, w)
            base = w * sigmoid(plain(po_in, k, r))
            if k == L - 1:
                base = base + act * rech_in[pl.ds(pl.multiple_of(r * T, T), T), :]
            put(r0, k, r, base)
        return c

    lax.fori_loop(0, R, local, 0)
    finish(0, NR0, 3 * T)

    def halo_rows(ref, st, base):
        for e, row in ((0, T - 1), (1, T + NX)):
            for k in range(L):
                ref[k, row:row + 1, :] = rrow[st, e, base + k:base + k + 1, :]

    halo_rows(pre, 0, 0)
    halo_rows(are, 0, L)
    for e, row in ((0, T - 1), (1, T + NX)):
        acte[0, row:row + 1, :] = rrow[0, e, 2 * L:2 * L + 1, :]
        for k in range(L):
            sre[k, row:row + 1, :] = sigmoid(rrow[0, e, k:k + 1, :])

    kl, kh = rcol[0, 0, T:2 * T, :], rcol[0, 1, T:2 * T, :]
    al, ah = rcol[0, 0, 2 * T:3 * T, :], rcol[0, 1, 2 * T:3 * T, :]

    def trans(r, c):
        act = tile(acte, 0, r)
        ha = 0.5 * act
        a_up = ha * up(acte, 0, r, act)
        a_dn = ha * down(acte, 0, r, act)
        a_lf = ha * left(act, al, 0, r)
        a_rt = ha * right(act, ah, 0, r)
        av = vertical_factor * ha * act
        cur = tile(are, 0, r)
        for k in range(L):
            put(txm, k, r, a_up * (cur + up(are, k, r, cur)))
            put(txp, k, r, a_dn * (cur + down(are, k, r, cur)))
            put(tym, k, r, a_lf * (cur + left(cur, kl, k, r)))
            put(typ, k, r, a_rt * (cur + right(cur, kh, k, r)))
            if k < L - 1:
                nxt = tile(are, k + 1, r)
                put(tzp, k, r, av * (cur + nxt))
                cur = nxt
        return c

    lax.fori_loop(0, R, trans, 0)

    pl_c, ph_c = rcol[0, 0, 0:T, :], rcol[0, 1, 0:T, :]
    shift = jnp.zeros((1, 1), f32)
    for it in range(NEWTON):
        sl_c, sh_c = sigmoid(pl_c), sigmoid(ph_c)

        def coef(r, acc):
            act = tile(acte, 0, r)
            rest = 1.0 - act
            pc, sc = tile(pre, 0, r), tile(sre, 0, r)
            below = None
            for k in range(L):
                s2 = sc * sc
                mc = 0.5 * s2
                s1 = 1.0 - sc
                ec = s2 * s1
                sm = sd = fl = None
                for pn, sn, tr, off in (
                    (up(pre, k, r, pc), up(sre, k, r, sc), txm, oxm),
                    (down(pre, k, r, pc), down(sre, k, r, sc), txp, oxp),
                    (left(pc, pl_c, k, r), left(sc, sl_c, k, r), tym, oym),
                    (right(pc, ph_c, k, r), right(sc, sh_c, k, r), typ, oyp),
                ):
                    n2 = sn * sn
                    t = plain(tr, k, r)
                    drop = pc - pn
                    tm = t * (mc + 0.5 * n2)
                    td = t * drop
                    put(off, k, r, n2 * (1.0 - sn) * td - tm)
                    if sm is None:
                        sm, sd, fl = tm, td, tm * drop
                    else:
                        sm, sd, fl = sm + tm, sd + td, fl + tm * drop
                if below is not None:
                    tm, td, f, eb = below
                    sm, sd, fl = sm + tm, sd - td, fl - f
                    put(ozm, k, r, -(eb * td + tm))
                if k < L - 1:
                    pn, sn = tile(pre, k + 1, r), tile(sre, k + 1, r)
                    n2 = sn * sn
                    t = plain(tzp, k, r)
                    drop = pc - pn - 1.0
                    tm = t * (mc + 0.5 * n2)
                    td = t * drop
                    f = tm * drop
                    put(ozp, k, r, n2 * (1.0 - sn) * td - tm)
                    sm, sd, fl = sm + tm, sd + td, fl + f
                    below = (tm, td, f, ec)
                w = plain(p9, k, r)
                put(dg, k, r, w * sc * s1 + rest + sm + ec * sd)
                q = plain(r0, k, r) - w * sc - fl - rest * pc
                put(are, k, r + 1, q)
                acc = pack(acc, q, k, r)
                if k < L - 1:
                    pc, sc = pn, sn
            return acc

        def send(ref, st, acc):
            for e, row in ((0, T), (1, T + NX - 1)):
                for k in range(L):
                    srow[st, e, k:k + 1, :] = ref[k, row:row + 1, :]
                scol[st, e, 0:T, :] = acc[e]
            start(st, NRL, T)

        def apply(ref, k, r, cur, before, after, lo, hi):
            y = plain(dg, k, r) * cur
            y = y + plain(oxm, k, r) * up(ref, k, r, cur)
            y = y + plain(oxp, k, r) * down(ref, k, r, cur)
            y = y + plain(oym, k, r) * left(cur, lo, k, r)
            y = y + plain(oyp, k, r) * right(cur, hi, k, r)
            if before is not None:
                y = y + plain(ozm, k, r) * before
            if after is not None:
                y = y + plain(ozp, k, r) * after
            return y - shift * cur

        st = 1 + 2 * it
        acc = lax.fori_loop(0, R, coef, z2)
        send(are, st, acc)
        finish(st, NRL, T)
        halo_rows(are, st, 0)
        a_lo, a_hi = rcol[st, 0, 0:T, :], rcol[st, 1, 0:T, :]

        def first(r, c):
            acc, aa, ab, bb = c
            before, cur = None, tile(are, 0, r)
            for k in range(L):
                after = tile(are, k + 1, r) if k < L - 1 else None
                b = apply(are, k, r, cur, before, after, a_lo, a_hi)
                put(bre, k, r + 1, b)
                acc = pack(acc, b, k, r)
                aa = aa + fold(cur * cur)
                ab = ab + fold(cur * b)
                bb = bb + fold(b * b)
                before, cur = cur, after
            return acc, aa, ab, bb

        acc, aa, ab, bb = lax.fori_loop(0, R, first, (z2, zero1, zero1, zero1))
        send(bre, st + 1, acc)
        finish(st + 1, NRL, T)
        halo_rows(bre, st + 1, 0)
        b_lo, b_hi = rcol[st + 1, 0, 0:T, :], rcol[st + 1, 1, 0:T, :]
        last = it == NEWTON - 1

        def second(r, c):
            ac, bc, cc = c
            before, cur = None, tile(bre, 0, r)
            for k in range(L):
                after = tile(bre, k + 1, r) if k < L - 1 else None
                v = apply(bre, k, r, cur, before, after, b_lo, b_hi)
                if last:
                    put(cre, k, r, v)
                ac = ac + fold(tile(are, k, r) * v)
                bc = bc + fold(cur * v)
                cc = cc + fold(v * v)
                before, cur = cur, after
            return ac, bc, cc

        ac, bc, cc = lax.fori_loop(0, R, second, (zero1, zero1, zero1))

        for i, v in enumerate((aa, ab, bb, ac, bc, cc)):
            sumy[it, 0, i:i + 1, :] = jnp.sum(v, axis=0, keepdims=True)
        for i in range(6, T):
            sumy[it, 0, i:i + 1, :] = jnp.zeros((1, W), f32)

        def spread(buf, n, mine, device, ss, rs):
            cps = []
            for d in range(1, n):
                c = pltpu.make_async_remote_copy(
                    src_ref=buf.at[it, 0], dst_ref=buf.at[it, d],
                    send_sem=ss.at[it, d], recv_sem=rs.at[it, d],
                    device_id=device(lax.rem(mine + d, n)), device_id_type=MESH)
                c.start()
                cps.append(c)
            for c in cps:
                c.wait()
            tot = buf[it, 0]
            for d in range(1, n):
                tot = tot + buf[it, d]
            return tot

        tot = spread(sumy, GY, gy, lambda o: (gx, o), ysend, yrecv)
        sumx[it, 0] = tot
        tot = spread(sumx, GX, gx, lambda o: (o, gy), xsend, xrecv)
        g = jnp.sum(tot, axis=1, keepdims=True)
        aa, ab, bb, ac, bc, cc = [g[i:i + 1, :] for i in range(6)]

        n2 = aa + epsilon
        n0 = jnp.sqrt(n2)
        dl = (ab - shift * epsilon) / n2
        h11 = shift + dl
        uu = jnp.maximum(bb - 2.0 * dl * ab + dl * dl * aa, 0.0) / n2
        h21s = uu + epsilon
        h21 = jnp.sqrt(h21s)
        ze = shift - dl
        zf = -dl * shift
        za = ac + ze * ab + zf * aa
        zb = bc + ze * bb + zf * ab
        zc = cc + ze * bc + zf * ac
        sc2 = n2 * h21s
        h12 = za / (n2 * h21)
        h22 = (zb - dl * za) / sc2
        zz = (zc + ze * zb + zf * za) / sc2
        v11 = aa / n2
        v22 = uu / h21s
        v12 = h11 * epsilon / (n2 * h21)
        u2 = zz - (2.0 - v11) * h12 * h12 - (2.0 - v22) * h22 * h22 + 2.0 * h12 * h22 * v12
        h32s = jnp.maximum(u2, 0.0) + epsilon
        r1 = jnp.sqrt(h11 * h11 + h21s)
        co, si = h11 / r1, h21 / r1
        tr = co * h12 + si * h22
        lo = co * h22 - si * h12
        y2 = -lo * si * n0 / (lo * lo + h32s)
        y1 = (co * n0 - tr * y2) / r1
        w1 = y1 / n0
        w2 = y2 / (n0 * h21)
        alpha, beta = w1 - w2 * dl, w2

        if not last:
            def step(r, c):
                for k in range(L):
                    p = plain(pre, k, r) + (alpha * plain(are, k, r) + beta * plain(bre, k, r))
                    put(pre, k, r, p)
                    put(sre, k, r, sigmoid(p))
                return c

            lax.fori_loop(0, R + 2, step, 0)
            pl_c = pl_c + (alpha * a_lo + beta * b_lo)
            ph_c = ph_c + (alpha * a_hi + beta * b_hi)
            shift = h11
        else:
            ga = 1.0 - w1 * shift - w2 * zf
            gb = w1 + w2 * ze
            def end(r, c):
                for k in range(L):
                    a, b = tile(are, k, r), tile(bre, k, r)
                    put(p_out, k, r, tile(pre, k, r) + (alpha * a + beta * b))
                    put(l_out, k, r, ga * a - gb * b - w2 * plain(cre, k, r))
                return c

            lax.fori_loop(0, R, end, 0)


def body(pressure, pressure_old, conductivity, porosity, recharge, active):
    L, NX, NY = pressure.shape
    GX, GY = lax.axis_size("gx"), lax.axis_size("gy")
    f32 = jnp.float32
    cell = pltpu.VMEM((L, NX, NY), f32)
    ext = pltpu.VMEM((L, NX + 2 * T, NY), f32)
    ST = 1 + 2 * NEWTON
    NR0 = ((2 * L + 1 + T - 1) // T) * T
    dma = pltpu.SemaphoreType.DMA
    vm = pl.BlockSpec(memory_space=pltpu.VMEM)
    return pl.pallas_call(
        functools.partial(kernel, L, NX, NY, GX, GY),
        out_shape=(jax.ShapeDtypeStruct(pressure.shape, f32),) * 2,
        in_specs=[vm] * 6,
        out_specs=(vm, vm),
        scratch_shapes=[ext] * 4 + [cell, pltpu.VMEM((1, NX + 2 * T, NY), f32), cell, cell]
        + [cell] * 5 + [cell] * 7
        + [
            pltpu.VMEM((ST, 2, NR0, NY), f32), pltpu.VMEM((ST, 2, 3 * T, W), f32),
            pltpu.VMEM((ST, 2, NR0, NY), f32), pltpu.VMEM((ST, 2, 3 * T, W), f32),
            pltpu.VMEM((NEWTON, GY, T, W), f32), pltpu.VMEM((NEWTON, GX, T, W), f32),
            dma((ST, 4)), dma((ST, 4)),
            dma((NEWTON, GY)), dma((NEWTON, GY)), dma((NEWTON, GX)), dma((NEWTON, GX)),
        ],
        compiler_params=pltpu.CompilerParams(
            collective_id=0, has_side_effects=True, vmem_limit_bytes=64000000
        ),
    )(pressure, pressure_old, conductivity, porosity, recharge, active)


def solution(mesh):
    cells, flat = P(None, "gx", "gy"), P("gx", "gy")
    return jax.shard_map(
        body,
        mesh=mesh,
        in_specs=(cells, cells, cells, cells, flat, flat),
        out_specs=(cells, cells),
        check_vma=False,
    )
```

```python
import functools

import jax
import jax.numpy as jnp
from jax import lax
from jax.experimental import pallas as pl
from jax.experimental.pallas import tpu as pltpu
from jax.sharding import PartitionSpec as P

NEWTON = 2
residual_sat = 0.1
vertical_factor = 2.0
epsilon = 1e-06
T = 8
W = 128
MESH = pl.DeviceIdType.MESH


def sigmoid(v):
    return 1.0 / (1.0 + jnp.exp(jnp.minimum(-v, 87.0)))


def fold(v):
    out = v[:, :W]
    for j in range(1, v.shape[1] // W):
        out = out + v[:, j * W:(j + 1) * W]
    return out


def kernel(
    L, NX, NY, GX, GY,
    p_hbm, po_hbm, k_hbm, por_hbm, rech_hbm, act_hbm,
    p_out, l_out,
    pre, sre, are, bre, cre, acte, p9, r0,
    txp, txm, typ, tym, tzp,
    dg, oxp, oxm, oyp, oym, ozp, ozm,
    srow, scol, rrow, rcol, sumy, sumx,
    act_in, rech_in, in_sem,
    send_sem, recv_sem, ysend, yrecv, xsend, xrecv,
):
    R = NX // T
    gx = lax.axis_index("gx")
    gy = lax.axis_index("gy")
    f32 = jnp.float32
    row8 = lax.broadcasted_iota(jnp.int32, (T, NY), 0)
    lane = lax.broadcasted_iota(jnp.int32, (T, NY), 1)
    lane1 = lax.broadcasted_iota(jnp.int32, (T, W), 1)
    has = (gx > 0, gx < GX - 1, gy > 0, gy < GY - 1)

    mid = pl.ds(T, NX)
    loads = [
        pltpu.make_async_copy(src, dst, in_sem.at[i])
        for i, (src, dst) in enumerate((
            (p_hbm, pre.at[:, mid, :]), (k_hbm, are.at[:, mid, :]), (act_hbm, act_in),
            (rech_hbm, rech_in), (por_hbm, p9), (po_hbm, r0),
        ))
    ]
    for c in loads:
        c.start()

    rrow[...] = jnp.zeros_like(rrow)
    rcol[...] = jnp.zeros_like(rcol)

    barrier = pltpu.get_barrier_semaphore()
    for d in range(1, GX):
        pl.semaphore_signal(barrier, inc=1, device_id=(lax.rem(gx + d, GX), gy), device_id_type=MESH)
    for d in range(1, GY):
        pl.semaphore_signal(barrier, inc=1, device_id=(gx, lax.rem(gy + d, GY)), device_id_type=MESH)

    def tile(ref, k, r):
        return ref[k, pl.ds(pl.multiple_of((r + 1) * T, T), T), :]

    def plain(ref, k, r):
        return ref[k, pl.ds(pl.multiple_of(r * T, T), T), :]

    def put(ref, k, r, v):
        ref[k, pl.ds(pl.multiple_of(r * T, T), T), :] = v

    def up(ref, k, r, cur):
        return pltpu.roll(jnp.where(row8 == T - 1, tile(ref, k, r - 1), cur), 1, 0)

    def down(ref, k, r, cur):
        return pltpu.roll(jnp.where(row8 == 0, tile(ref, k, r + 1), cur), T - 1, 0)

    def wide(v):
        return jnp.concatenate([v] * (NY // W), axis=1)

    def left(cur, halo, k, r):
        h = pltpu.roll(halo, lax.rem(2 * W - (k * R + r), W), 1)
        return jnp.where(lane == 0, wide(h), pltpu.roll(cur, 1, 1))

    def right(cur, halo, k, r):
        h = pltpu.roll(halo, W - 1 - (k * R + r), 1)
        return jnp.where(lane == NY - 1, wide(h), pltpu.roll(cur, NY - 1, 1))

    def pack(acc, v, k, r):
        lo, hi = acc
        at = lane1 == k * R + r
        lo = jnp.where(at, jnp.broadcast_to(v[:, 0:1], (T, W)), lo)
        hi = jnp.where(at, jnp.broadcast_to(v[:, NY - 1:NY], (T, W)), hi)
        return lo, hi

    zero1 = jnp.zeros((T, W), f32)

    peers = ((gx - 1, gy), (gx + 1, gy), (gx, gy - 1), (gx, gy + 1))

    def copies(st, part, n):
        out = []
        for d in (0, 1) if part == 0 else (2, 3):
            back = d ^ 1
            if part == 0:
                src, dst = srow.at[st, d, pl.ds(0, n)], rrow.at[st, back, pl.ds(0, n)]
            else:
                src = scol.at[st, part - 1, d - 2, pl.ds(0, n)]
                dst = rcol.at[st, part - 1, back - 2, pl.ds(0, n)]
            out.append((has[d], has[back], pltpu.make_async_remote_copy(
                src_ref=src, dst_ref=dst,
                send_sem=send_sem.at[st, part, d % 2], recv_sem=recv_sem.at[st, part, back % 2],
                device_id=peers[d], device_id_type=MESH)))
        return out

    def start(st, part, n):
        for to, _, c in copies(st, part, n):
            @pl.when(to)
            def _(c=c):
                c.start()

    sent = []

    def recv(st, part, n, also=True):
        sent.append((st, part, n))
        for _, frm, c in copies(st, part, n):
            @pl.when(jnp.logical_and(frm, also))
            def _(c=c):
                c.wait_recv()

    NR0 = srow.shape[2]
    NRL = ((L + T - 1) // T) * T

    for c in loads[:3]:
        c.wait()

    for e, row in ((0, 0), (1, NX - 1)):
        for k in range(L):
            srow[0, e, k:k + 1, :] = pre[k, T + row:T + row + 1, :]
            srow[0, e, L + k:L + k + 1, :] = are[k, T + row:T + row + 1, :]
        srow[0, e, 2 * L:2 * L + 1, :] = act_in[row:row + 1, :].astype(f32)

    def pack0(r, c):
        pp, kk, aa = c
        for k in range(L):
            pp = pack(pp, tile(pre, k, r), k, r)
            kk = pack(kk, tile(are, k, r), k, r)
        aa = pack(aa, act_in[pl.ds(pl.multiple_of(r * T, T), T), :].astype(f32), 0, r)
        return pp, kk, aa

    z2 = (zero1, zero1)
    pp, kk, aa = lax.fori_loop(0, R, pack0, (z2, z2, z2))
    for e in range(2):
        scol[0, 0, e, 0:T, :] = pp[e]
        scol[0, 0, e, T:2 * T, :] = kk[e]
        scol[0, 0, e, 2 * T:3 * T, :] = aa[e]
    pl.semaphore_wait(barrier, GX - 1 + GY - 1)
    start(0, 0, NR0)
    start(0, 1, 3 * T)
    for c in loads[3:]:
        c.wait()

    def local(r, c):
        act = act_in[pl.ds(pl.multiple_of(r * T, T), T), :].astype(f32)
        put(acte, 0, r + 1, act)
        for k in range(L):
            put(sre, k, r + 1, sigmoid(tile(pre, k, r)))
            w = (1.0 - residual_sat) * act * plain(p9, k, r)
            put(p9, k, r, w)
            base = w * sigmoid(plain(r0, k, r))
            if k == L - 1:
                base = base + act * rech_in[pl.ds(pl.multiple_of(r * T, T), T), :]
            put(r0, k, r, base)
        return c

    lax.fori_loop(0, R, local, 0)
    recv(0, 0, NR0)
    recv(0, 1, 3 * T)

    def halo_rows(ref, st, base):
        for e, row in ((0, T - 1), (1, T + NX)):
            for k in range(L):
                ref[k, row:row + 1, :] = rrow[st, e, base + k:base + k + 1, :]

    halo_rows(pre, 0, 0)
    halo_rows(are, 0, L)
    for e, row in ((0, T - 1), (1, T + NX)):
        acte[0, row:row + 1, :] = rrow[0, e, 2 * L:2 * L + 1, :]
        for k in range(L):
            sre[k, row:row + 1, :] = sigmoid(rrow[0, e, k:k + 1, :])

    kl, kh = rcol[0, 0, 0, T:2 * T, :], rcol[0, 0, 1, T:2 * T, :]
    al, ah = rcol[0, 0, 0, 2 * T:3 * T, :], rcol[0, 0, 1, 2 * T:3 * T, :]

    def trans(r, c):
        act = tile(acte, 0, r)
        ha = 0.5 * act
        a_up = ha * up(acte, 0, r, act)
        a_dn = ha * down(acte, 0, r, act)
        a_lf = ha * left(act, al, 0, r)
        a_rt = ha * right(act, ah, 0, r)
        av = vertical_factor * ha * act
        cur = tile(are, 0, r)
        for k in range(L):
            put(txm, k, r, a_up * (cur + up(are, k, r, cur)))
            put(txp, k, r, a_dn * (cur + down(are, k, r, cur)))
            put(tym, k, r, a_lf * (cur + left(cur, kl, k, r)))
            put(typ, k, r, a_rt * (cur + right(cur, kh, k, r)))
            if k < L - 1:
                nxt = tile(are, k + 1, r)
                put(tzp, k, r, av * (cur + nxt))
                cur = nxt
        return c

    lax.fori_loop(0, R, trans, 0)

    pl_c, ph_c = rcol[0, 0, 0, 0:T, :], rcol[0, 0, 1, 0:T, :]
    shift = jnp.zeros((1, 1), f32)
    H = max(2, R - 3)

    def order(i):
        return jnp.where(i < 2, i * (R - 1), i - 1)

    def emit(ref, st, i, acc):
        @pl.when(i == 1)
        def _():
            for e, row in ((0, T), (1, T + NX - 1)):
                for k in range(L):
                    srow[st, e, k:k + 1, :] = ref[k, row:row + 1, :]
            start(st, 0, NRL)

        for part, at in ((1, H - 1), (2, R - 1)):
            @pl.when(i == at)
            def _(part=part):
                scol[st, part - 1, 0, 0:T, :] = acc[0]
                scol[st, part - 1, 1, 0:T, :] = acc[1]
                start(st, part, T)

    def ready(st, i):
        recv(st, 2, T, i == H)

    def halo(st, i):
        late = jnp.where(i < H, 0, 1)
        return rcol[st, late, 0, 0:T, :], rcol[st, late, 1, 0:T, :]

    for it in range(NEWTON):
        sl_c, sh_c = sigmoid(pl_c), sigmoid(ph_c)

        st = 1 + 2 * it

        def coef(i, acc):
            r = order(i)
            act = tile(acte, 0, r)
            rest = 1.0 - act
            pc, sc = tile(pre, 0, r), tile(sre, 0, r)
            below = None
            for k in range(L):
                s2 = sc * sc
                mc = 0.5 * s2
                s1 = 1.0 - sc
                ec = s2 * s1
                sm = sd = fl = None
                for pn, sn, tr, off in (
                    (up(pre, k, r, pc), up(sre, k, r, sc), txm, oxm),
                    (down(pre, k, r, pc), down(sre, k, r, sc), txp, oxp),
                    (left(pc, pl_c, k, r), left(sc, sl_c, k, r), tym, oym),
                    (right(pc, ph_c, k, r), right(sc, sh_c, k, r), typ, oyp),
                ):
                    n2 = sn * sn
                    t = plain(tr, k, r)
                    drop = pc - pn
                    tm = t * (mc + 0.5 * n2)
                    td = t * drop
                    put(off, k, r, n2 * (1.0 - sn) * td - tm)
                    if sm is None:
                        sm, sd, fl = tm, td, tm * drop
                    else:
                        sm, sd, fl = sm + tm, sd + td, fl + tm * drop
                if below is not None:
                    tm, td, f, eb = below
                    sm, sd, fl = sm + tm, sd - td, fl - f
                    put(ozm, k, r, -(eb * td + tm))
                if k < L - 1:
                    pn, sn = tile(pre, k + 1, r), tile(sre, k + 1, r)
                    n2 = sn * sn
                    t = plain(tzp, k, r)
                    drop = pc - pn - 1.0
                    tm = t * (mc + 0.5 * n2)
                    td = t * drop
                    f = tm * drop
                    put(ozp, k, r, n2 * (1.0 - sn) * td - tm)
                    sm, sd, fl = sm + tm, sd + td, fl + f
                    below = (tm, td, f, ec)
                w = plain(p9, k, r)
                put(dg, k, r, w * sc * s1 + rest + sm + ec * sd)
                q = plain(r0, k, r) - w * sc - fl - rest * pc
                put(are, k, r + 1, q)
                acc = pack(acc, q, k, r)
                if k < L - 1:
                    pc, sc = pn, sn
            emit(are, st, i, acc)
            return acc

        def apply(ref, k, r, cur, before, after, lo, hi):
            y = plain(dg, k, r) * cur
            y = y + plain(oxm, k, r) * up(ref, k, r, cur)
            y = y + plain(oxp, k, r) * down(ref, k, r, cur)
            y = y + plain(oym, k, r) * left(cur, lo, k, r)
            y = y + plain(oyp, k, r) * right(cur, hi, k, r)
            if before is not None:
                y = y + plain(ozm, k, r) * before
            if after is not None:
                y = y + plain(ozp, k, r) * after
            return y - shift * cur

        lax.fori_loop(0, R, coef, z2)
        recv(st, 0, NRL)
        recv(st, 1, T)
        halo_rows(are, st, 0)

        def first(i, c):
            r = order(i)
            ready(st, i)
            a_lo, a_hi = halo(st, i)
            acc, aa, ab, bb = c
            before, cur = None, tile(are, 0, r)
            for k in range(L):
                after = tile(are, k + 1, r) if k < L - 1 else None
                b = apply(are, k, r, cur, before, after, a_lo, a_hi)
                put(bre, k, r + 1, b)
                acc = pack(acc, b, k, r)
                aa = aa + fold(cur * cur)
                ab = ab + fold(cur * b)
                bb = bb + fold(b * b)
                before, cur = cur, after
            emit(bre, st + 1, i, acc)
            return acc, aa, ab, bb

        acc, aa, ab, bb = lax.fori_loop(0, R, first, (z2, zero1, zero1, zero1))
        recv(st + 1, 0, NRL)
        recv(st + 1, 1, T)
        halo_rows(bre, st + 1, 0)
        last = it == NEWTON - 1

        def second(i, c):
            r = order(i)
            ready(st + 1, i)
            b_lo, b_hi = halo(st + 1, i)
            ac, bc, cc = c
            before, cur = None, tile(bre, 0, r)
            for k in range(L):
                after = tile(bre, k + 1, r) if k < L - 1 else None
                v = apply(bre, k, r, cur, before, after, b_lo, b_hi)
                if last:
                    put(cre, k, r, v)
                ac = ac + fold(tile(are, k, r) * v)
                bc = bc + fold(cur * v)
                cc = cc + fold(v * v)
                before, cur = cur, after
            return ac, bc, cc

        ac, bc, cc = lax.fori_loop(0, R, second, (zero1, zero1, zero1))

        for i, v in enumerate((aa, ab, bb, ac, bc, cc)):
            sumy[it, 0, i:i + 1, :] = jnp.sum(v, axis=0, keepdims=True)
        for i in range(6, T):
            sumy[it, 0, i:i + 1, :] = jnp.zeros((1, W), f32)

        def spread(buf, n, mine, device, ss, rs):
            cps = []
            for d in range(1, n):
                c = pltpu.make_async_remote_copy(
                    src_ref=buf.at[it, 0], dst_ref=buf.at[it, d],
                    send_sem=ss.at[it, d], recv_sem=rs.at[it, d],
                    device_id=device(lax.rem(mine + d, n)), device_id_type=MESH)
                c.start()
                cps.append(c)
            for c in cps:
                c.wait()
            tot = buf[it, 0]
            for d in range(1, n):
                tot = tot + buf[it, d]
            return tot

        tot = spread(sumy, GY, gy, lambda o: (gx, o), ysend, yrecv)
        sumx[it, 0] = tot
        tot = spread(sumx, GX, gx, lambda o: (o, gy), xsend, xrecv)
        g = jnp.sum(tot, axis=1, keepdims=True)
        aa, ab, bb, ac, bc, cc = [g[i:i + 1, :] for i in range(6)]

        n2 = aa + epsilon
        n0 = jnp.sqrt(n2)
        dl = (ab - shift * epsilon) / n2
        h11 = shift + dl
        uu = jnp.maximum(bb - 2.0 * dl * ab + dl * dl * aa, 0.0) / n2
        h21s = uu + epsilon
        h21 = jnp.sqrt(h21s)
        ze = shift - dl
        zf = -dl * shift
        za = ac + ze * ab + zf * aa
        zb = bc + ze * bb + zf * ab
        zc = cc + ze * bc + zf * ac
        sc2 = n2 * h21s
        h12 = za / (n2 * h21)
        h22 = (zb - dl * za) / sc2
        zz = (zc + ze * zb + zf * za) / sc2
        v11 = aa / n2
        v22 = uu / h21s
        v12 = h11 * epsilon / (n2 * h21)
        u2 = zz - (2.0 - v11) * h12 * h12 - (2.0 - v22) * h22 * h22 + 2.0 * h12 * h22 * v12
        h32s = jnp.maximum(u2, 0.0) + epsilon
        r1 = jnp.sqrt(h11 * h11 + h21s)
        co, si = h11 / r1, h21 / r1
        tr = co * h12 + si * h22
        lo = co * h22 - si * h12
        y2 = -lo * si * n0 / (lo * lo + h32s)
        y1 = (co * n0 - tr * y2) / r1
        w1 = y1 / n0
        w2 = y2 / (n0 * h21)
        alpha, beta = w1 - w2 * dl, w2

        if not last:
            def step(r, c):
                for k in range(L):
                    p = plain(pre, k, r) + (alpha * plain(are, k, r) + beta * plain(bre, k, r))
                    put(pre, k, r, p)
                    put(sre, k, r, sigmoid(p))
                return c

            lax.fori_loop(0, R + 2, step, 0)
            (a_lo, a_hi), (b_lo, b_hi) = halo(st, R), halo(st + 1, R)
            pl_c = pl_c + (alpha * a_lo + beta * b_lo)
            ph_c = ph_c + (alpha * a_hi + beta * b_hi)
            shift = h11
        else:
            ga = 1.0 - w1 * shift - w2 * zf
            gb = w1 + w2 * ze
            def end(r, c):
                for k in range(L):
                    a, b = tile(are, k, r), tile(bre, k, r)
                    put(p_out, k, r, tile(pre, k, r) + (alpha * a + beta * b))
                    put(l_out, k, r, ga * a - gb * b - w2 * plain(cre, k, r))
                return c

            lax.fori_loop(0, R, end, 0)

    for st, part, n in sent:
        for to, _, c in copies(st, part, n):
            @pl.when(to)
            def _(c=c):
                c.wait_send()


def body(pressure, pressure_old, conductivity, porosity, recharge, active):
    L, NX, NY = pressure.shape
    GX, GY = lax.axis_size("gx"), lax.axis_size("gy")
    f32 = jnp.float32
    cell = pltpu.VMEM((L, NX, NY), f32)
    ext = pltpu.VMEM((L, NX + 2 * T, NY), f32)
    ST = 1 + 2 * NEWTON
    NR0 = ((2 * L + 1 + T - 1) // T) * T
    dma = pltpu.SemaphoreType.DMA
    vm = pl.BlockSpec(memory_space=pltpu.VMEM)
    return pl.pallas_call(
        functools.partial(kernel, L, NX, NY, GX, GY),
        out_shape=(jax.ShapeDtypeStruct(pressure.shape, f32),) * 2,
        in_specs=[pl.BlockSpec(memory_space=pl.ANY)] * 6,
        out_specs=(vm, vm),
        scratch_shapes=[ext] * 4 + [cell, pltpu.VMEM((1, NX + 2 * T, NY), f32), cell, cell]
        + [cell] * 5 + [cell] * 7
        + [
            pltpu.VMEM((ST, 2, NR0, NY), f32), pltpu.VMEM((ST, 2, 2, 3 * T, W), f32),
            pltpu.VMEM((ST, 2, NR0, NY), f32), pltpu.VMEM((ST, 2, 2, 3 * T, W), f32),
            pltpu.VMEM((NEWTON, GY, T, W), f32), pltpu.VMEM((NEWTON, GX, T, W), f32),
            pltpu.VMEM((NX, NY), jnp.int32), pltpu.VMEM((NX, NY), f32), dma((6,)),
            dma((ST, 3, 2)), dma((ST, 3, 2)),
            dma((NEWTON, GY)), dma((NEWTON, GY)), dma((NEWTON, GX)), dma((NEWTON, GX)),
        ],
        compiler_params=pltpu.CompilerParams(
            collective_id=0, has_side_effects=True, vmem_limit_bytes=64000000
        ),
    )(pressure, pressure_old, conductivity, porosity, recharge, active)


def solution(mesh):
    cells, flat = P(None, "gx", "gy"), P("gx", "gy")
    return jax.shard_map(
        body,
        mesh=mesh,
        in_specs=(cells, cells, cells, cells, flat, flat),
        out_specs=(cells, cells),
        check_vma=False,
    )
```

```python
import functools

import jax
import jax.numpy as jnp
from jax import lax
from jax.experimental import pallas as pl
from jax.experimental.pallas import tpu as pltpu
from jax.sharding import PartitionSpec as P

NEWTON = 2
residual_sat = 0.1
vertical_factor = 2.0
epsilon = 1e-06
T = 8
W = 128
MESH = pl.DeviceIdType.MESH


def sigmoid(v):
    return 1.0 / (1.0 + jnp.exp(jnp.minimum(-v, 87.0)))


def fold(v):
    out = v[:, :W]
    for j in range(1, v.shape[1] // W):
        out = out + v[:, j * W:(j + 1) * W]
    return out


def kernel(
    L, NX, NY, GX, GY,
    p_hbm, po_hbm, k_hbm, por_hbm, rech_hbm, act_hbm,
    pre, are, bre, cre, fin,
    sre, acte, p9, r0,
    txp, txm, typ, tym, tzp,
    dg, oxp, oxm, oyp, oym, ozp, ozm,
    srow, scol, rrow, rcol, sumy, sumx,
    act_in, rech_in, in_sem,
    send_sem, recv_sem, ysend, yrecv, xsend, xrecv,
):
    R = NX // T
    gx = lax.axis_index("gx")
    gy = lax.axis_index("gy")
    f32 = jnp.float32
    row8 = lax.broadcasted_iota(jnp.int32, (T, NY), 0)
    lane = lax.broadcasted_iota(jnp.int32, (T, NY), 1)
    lane1 = lax.broadcasted_iota(jnp.int32, (T, W), 1)
    has = (gx > 0, gx < GX - 1, gy > 0, gy < GY - 1)

    mid = pl.ds(T, NX)
    loads = [
        pltpu.make_async_copy(src, dst, in_sem.at[i])
        for i, (src, dst) in enumerate((
            (p_hbm, pre.at[:, mid, :]), (k_hbm, are.at[:, mid, :]), (act_hbm, act_in),
            (rech_hbm, rech_in), (por_hbm, p9), (po_hbm, r0),
        ))
    ]
    for c in loads:
        c.start()

    rrow[...] = jnp.zeros_like(rrow)
    rcol[...] = jnp.zeros_like(rcol)

    barrier = pltpu.get_barrier_semaphore()
    for d in range(1, GX):
        pl.semaphore_signal(barrier, inc=1, device_id=(lax.rem(gx + d, GX), gy), device_id_type=MESH)
    for d in range(1, GY):
        pl.semaphore_signal(barrier, inc=1, device_id=(gx, lax.rem(gy + d, GY)), device_id_type=MESH)

    def tile(ref, k, r):
        return ref[k, pl.ds(pl.multiple_of((r + 1) * T, T), T), :]

    def plain(ref, k, r):
        return ref[k, pl.ds(pl.multiple_of(r * T, T), T), :]

    def put(ref, k, r, v):
        ref[k, pl.ds(pl.multiple_of(r * T, T), T), :] = v

    def up(ref, k, r, cur):
        return pltpu.roll(jnp.where(row8 == T - 1, tile(ref, k, r - 1), cur), 1, 0)

    def down(ref, k, r, cur):
        return pltpu.roll(jnp.where(row8 == 0, tile(ref, k, r + 1), cur), T - 1, 0)

    def wide(v):
        return jnp.concatenate([v] * (NY // W), axis=1)

    def left(cur, halo, k, r):
        h = pltpu.roll(halo, lax.rem(W + 1 - (k * R + r), W), 1)
        return jnp.where(lane == 0, wide(h), pltpu.roll(cur, 1, 1))

    def right(cur, halo, k, r):
        h = pltpu.roll(halo, W - 1 - (k * R + r), 1)
        return jnp.where(lane == NY - 1, wide(h), pltpu.roll(cur, NY - 1, 1))

    def pack(acc, v, k, r):
        lo, hi = acc
        both = jnp.where(lane1 == 0, v[:, :W], v[:, NY - W:])
        both = pltpu.roll(both, k * R + r, 1)
        lo = jnp.where(lane1 == k * R + r, both, lo)
        hi = jnp.where(lane1 == lax.rem(k * R + r + W - 1, W), both, hi)
        return lo, hi

    zero1 = jnp.zeros((T, W), f32)

    peers = ((gx - 1, gy), (gx + 1, gy), (gx, gy - 1), (gx, gy + 1))

    def copies(st, part, n):
        out = []
        for d in (0, 1) if part == 0 else (2, 3):
            back = d ^ 1
            if part == 0:
                src, dst = srow.at[st, d, pl.ds(0, n)], rrow.at[st, back, pl.ds(0, n)]
            else:
                src = scol.at[st, part - 1, d - 2, pl.ds(0, n)]
                dst = rcol.at[st, part - 1, back - 2, pl.ds(0, n)]
            out.append((has[d], has[back], pltpu.make_async_remote_copy(
                src_ref=src, dst_ref=dst,
                send_sem=send_sem.at[st, part, d % 2], recv_sem=recv_sem.at[st, part, back % 2],
                device_id=peers[d], device_id_type=MESH)))
        return out

    def start(st, part, n):
        for to, _, c in copies(st, part, n):
            @pl.when(to)
            def _(c=c):
                c.start()

    sent = []

    def recv(st, part, n, also=True):
        sent.append((st, part, n))
        for _, frm, c in copies(st, part, n):
            @pl.when(jnp.logical_and(frm, also))
            def _(c=c):
                c.wait_recv()

    NR0 = srow.shape[2]
    NRL = ((L + T - 1) // T) * T

    for c in loads[:3]:
        c.wait()

    for e, row in ((0, 0), (1, NX - 1)):
        for k in range(L):
            srow[0, e, k:k + 1, :] = pre[k, T + row:T + row + 1, :]
            srow[0, e, L + k:L + k + 1, :] = are[k, T + row:T + row + 1, :]
        srow[0, e, 2 * L:2 * L + 1, :] = act_in[row:row + 1, :].astype(f32)

    def pack0(r, c):
        pp, kk, aa = c
        for k in range(L):
            pp = pack(pp, tile(pre, k, r), k, r)
            kk = pack(kk, tile(are, k, r), k, r)
        aa = pack(aa, act_in[pl.ds(pl.multiple_of(r * T, T), T), :].astype(f32), 0, r)
        return pp, kk, aa

    z2 = (zero1, zero1)
    pp, kk, aa = lax.fori_loop(0, R, pack0, (z2, z2, z2))
    for e in range(2):
        scol[0, 0, e, 0:T, :] = pp[e]
        scol[0, 0, e, T:2 * T, :] = kk[e]
        scol[0, 0, e, 2 * T:3 * T, :] = aa[e]
    pl.semaphore_wait(barrier, GX - 1 + GY - 1)
    start(0, 0, NR0)
    start(0, 1, 3 * T)
    for c in loads[3:]:
        c.wait()

    def local(r, c):
        act = act_in[pl.ds(pl.multiple_of(r * T, T), T), :].astype(f32)
        put(acte, 0, r + 1, act)
        for k in range(L):
            put(sre, k, r + 1, sigmoid(tile(pre, k, r)))
            w = (1.0 - residual_sat) * act * plain(p9, k, r)
            put(p9, k, r, w)
            base = w * sigmoid(plain(r0, k, r))
            if k == L - 1:
                base = base + act * rech_in[pl.ds(pl.multiple_of(r * T, T), T), :]
            put(r0, k, r, base)
        return c

    lax.fori_loop(0, R, local, 0)
    recv(0, 0, NR0)
    recv(0, 1, 3 * T)

    def halo_rows(ref, st, base):
        for e, row in ((0, T - 1), (1, T + NX)):
            for k in range(L):
                ref[k, row:row + 1, :] = rrow[st, e, base + k:base + k + 1, :]

    halo_rows(pre, 0, 0)
    halo_rows(are, 0, L)
    for e, row in ((0, T - 1), (1, T + NX)):
        acte[0, row:row + 1, :] = rrow[0, e, 2 * L:2 * L + 1, :]
        for k in range(L):
            sre[k, row:row + 1, :] = sigmoid(rrow[0, e, k:k + 1, :])

    kl, kh = rcol[0, 0, 0, T:2 * T, :], rcol[0, 0, 1, T:2 * T, :]
    al, ah = rcol[0, 0, 0, 2 * T:3 * T, :], rcol[0, 0, 1, 2 * T:3 * T, :]

    def trans(r, c):
        act = tile(acte, 0, r)
        ha = 0.5 * act
        a_up = ha * up(acte, 0, r, act)
        a_dn = ha * down(acte, 0, r, act)
        a_lf = ha * left(act, al, 0, r)
        a_rt = ha * right(act, ah, 0, r)
        av = vertical_factor * ha * act
        cur = tile(are, 0, r)
        for k in range(L):
            put(txm, k, r, a_up * (cur + up(are, k, r, cur)))
            put(txp, k, r, a_dn * (cur + down(are, k, r, cur)))
            put(tym, k, r, a_lf * (cur + left(cur, kl, k, r)))
            put(typ, k, r, a_rt * (cur + right(cur, kh, k, r)))
            if k < L - 1:
                nxt = tile(are, k + 1, r)
                put(tzp, k, r, av * (cur + nxt))
                cur = nxt
        return c

    lax.fori_loop(0, R, trans, 0)

    pl_c, ph_c = rcol[0, 0, 0, 0:T, :], rcol[0, 0, 1, 0:T, :]
    shift = jnp.zeros((1, 1), f32)
    H = max(2, R - 3)

    def order(i):
        return jnp.where(i < 2, i * (R - 1), i - 1)

    def emit(ref, st, i, acc):
        @pl.when(i == 1)
        def _():
            for e, row in ((0, T), (1, T + NX - 1)):
                for k in range(L):
                    srow[st, e, k:k + 1, :] = ref[k, row:row + 1, :]
            start(st, 0, NRL)

        for part, at in ((1, H - 1), (2, R - 1)):
            @pl.when(i == at)
            def _(part=part):
                scol[st, part - 1, 0, 0:T, :] = acc[0]
                scol[st, part - 1, 1, 0:T, :] = acc[1]
                start(st, part, T)

    def ready(st, i):
        recv(st, 2, T, i == H)

    def halo(st, i):
        late = jnp.where(i < H, 0, 1)
        return rcol[st, late, 0, 0:T, :], rcol[st, late, 1, 0:T, :]

    for it in range(NEWTON):
        sl_c, sh_c = sigmoid(pl_c), sigmoid(ph_c)

        st = 1 + 2 * it

        def coef(i, acc):
            r = order(i)
            act = tile(acte, 0, r)
            rest = 1.0 - act
            pc, sc = tile(pre, 0, r), tile(sre, 0, r)
            below = None
            for k in range(L):
                s2 = sc * sc
                mc = 0.5 * s2
                s1 = 1.0 - sc
                ec = s2 * s1
                sm = sd = fl = None
                for pn, sn, tr, off in (
                    (up(pre, k, r, pc), up(sre, k, r, sc), txm, oxm),
                    (down(pre, k, r, pc), down(sre, k, r, sc), txp, oxp),
                    (left(pc, pl_c, k, r), left(sc, sl_c, k, r), tym, oym),
                    (right(pc, ph_c, k, r), right(sc, sh_c, k, r), typ, oyp),
                ):
                    n2 = sn * sn
                    t = plain(tr, k, r)
                    drop = pc - pn
                    tm = t * (mc + 0.5 * n2)
                    td = t * drop
                    put(off, k, r, n2 * (1.0 - sn) * td - tm)
                    if sm is None:
                        sm, sd, fl = tm, td, tm * drop
                    else:
                        sm, sd, fl = sm + tm, sd + td, fl + tm * drop
                if below is not None:
                    tm, td, f, eb = below
                    sm, sd, fl = sm + tm, sd - td, fl - f
                    put(ozm, k, r, -(eb * td + tm))
                if k < L - 1:
                    pn, sn = tile(pre, k + 1, r), tile(sre, k + 1, r)
                    n2 = sn * sn
                    t = plain(tzp, k, r)
                    drop = pc - pn - 1.0
                    tm = t * (mc + 0.5 * n2)
                    td = t * drop
                    f = tm * drop
                    put(ozp, k, r, n2 * (1.0 - sn) * td - tm)
                    sm, sd, fl = sm + tm, sd + td, fl + f
                    below = (tm, td, f, ec)
                w = plain(p9, k, r)
                put(dg, k, r, w * sc * s1 + rest + sm + ec * sd)
                q = plain(r0, k, r) - w * sc - fl - rest * pc
                put(are, k, r + 1, q)
                acc = pack(acc, q, k, r)
                if k < L - 1:
                    pc, sc = pn, sn
            emit(are, st, i, acc)
            return acc

        def apply(ref, k, r, cur, before, after, lo, hi):
            y = plain(dg, k, r) * cur
            y = y + plain(oxm, k, r) * up(ref, k, r, cur)
            y = y + plain(oxp, k, r) * down(ref, k, r, cur)
            y = y + plain(oym, k, r) * left(cur, lo, k, r)
            y = y + plain(oyp, k, r) * right(cur, hi, k, r)
            if before is not None:
                y = y + plain(ozm, k, r) * before
            if after is not None:
                y = y + plain(ozp, k, r) * after
            return y - shift * cur

        lax.fori_loop(0, R, coef, z2)
        recv(st, 0, NRL)
        recv(st, 1, T)
        halo_rows(are, st, 0)

        def first(i, c):
            r = order(i)
            ready(st, i)
            a_lo, a_hi = halo(st, i)
            acc, aa, ab, bb = c
            before, cur = None, tile(are, 0, r)
            for k in range(L):
                after = tile(are, k + 1, r) if k < L - 1 else None
                b = apply(are, k, r, cur, before, after, a_lo, a_hi)
                put(bre, k, r + 1, b)
                acc = pack(acc, b, k, r)
                aa = aa + fold(cur * cur)
                ab = ab + fold(cur * b)
                bb = bb + fold(b * b)
                before, cur = cur, after
            emit(bre, st + 1, i, acc)
            return acc, aa, ab, bb

        acc, aa, ab, bb = lax.fori_loop(0, R, first, (z2, zero1, zero1, zero1))
        recv(st + 1, 0, NRL)
        recv(st + 1, 1, T)
        halo_rows(bre, st + 1, 0)
        last = it == NEWTON - 1

        def second(i, c):
            r = order(i)
            ready(st + 1, i)
            b_lo, b_hi = halo(st + 1, i)
            ac, bc, cc = c
            before, cur = None, tile(bre, 0, r)
            for k in range(L):
                after = tile(bre, k + 1, r) if k < L - 1 else None
                v = apply(bre, k, r, cur, before, after, b_lo, b_hi)
                if last:
                    put(cre, k, r, v)
                ac = ac + fold(tile(are, k, r) * v)
                bc = bc + fold(cur * v)
                cc = cc + fold(v * v)
                before, cur = cur, after
            return ac, bc, cc

        ac, bc, cc = lax.fori_loop(0, R, second, (zero1, zero1, zero1))

        for i, v in enumerate((aa, ab, bb, ac, bc, cc)):
            sumy[it, 0, i:i + 1, :] = jnp.sum(v, axis=0, keepdims=True)
        for i in range(6, T):
            sumy[it, 0, i:i + 1, :] = jnp.zeros((1, W), f32)

        def spread(buf, n, mine, device, ss, rs):
            cps = []
            for d in range(1, n):
                c = pltpu.make_async_remote_copy(
                    src_ref=buf.at[it, 0], dst_ref=buf.at[it, d],
                    send_sem=ss.at[it, d], recv_sem=rs.at[it, d],
                    device_id=device(lax.rem(mine + d, n)), device_id_type=MESH)
                c.start()
                cps.append(c)
            for c in cps:
                c.wait()
            tot = buf[it, 0]
            for d in range(1, n):
                tot = tot + buf[it, d]
            return tot

        tot = spread(sumy, GY, gy, lambda o: (gx, o), ysend, yrecv)
        sumx[it, 0] = tot
        tot = spread(sumx, GX, gx, lambda o: (o, gy), xsend, xrecv)
        g = jnp.sum(tot, axis=1, keepdims=True)
        aa, ab, bb, ac, bc, cc = [g[i:i + 1, :] for i in range(6)]

        n2 = aa + epsilon
        n0 = jnp.sqrt(n2)
        dl = (ab - shift * epsilon) / n2
        h11 = shift + dl
        uu = jnp.maximum(bb - 2.0 * dl * ab + dl * dl * aa, 0.0) / n2
        h21s = uu + epsilon
        h21 = jnp.sqrt(h21s)
        ze = shift - dl
        zf = -dl * shift
        za = ac + ze * ab + zf * aa
        zb = bc + ze * bb + zf * ab
        zc = cc + ze * bc + zf * ac
        sc2 = n2 * h21s
        h12 = za / (n2 * h21)
        h22 = (zb - dl * za) / sc2
        zz = (zc + ze * zb + zf * za) / sc2
        v11 = aa / n2
        v22 = uu / h21s
        v12 = h11 * epsilon / (n2 * h21)
        u2 = zz - (2.0 - v11) * h12 * h12 - (2.0 - v22) * h22 * h22 + 2.0 * h12 * h22 * v12
        h32s = jnp.maximum(u2, 0.0) + epsilon
        r1 = jnp.sqrt(h11 * h11 + h21s)
        co, si = h11 / r1, h21 / r1
        tr = co * h12 + si * h22
        lo = co * h22 - si * h12
        y2 = -lo * si * n0 / (lo * lo + h32s)
        y1 = (co * n0 - tr * y2) / r1
        w1 = y1 / n0
        w2 = y2 / (n0 * h21)
        alpha, beta = w1 - w2 * dl, w2

        if not last:
            def step(r, c):
                for k in range(L):
                    p = plain(pre, k, r) + (alpha * plain(are, k, r) + beta * plain(bre, k, r))
                    put(pre, k, r, p)
                    put(sre, k, r, sigmoid(p))
                return c

            lax.fori_loop(0, R + 2, step, 0)
            (a_lo, a_hi), (b_lo, b_hi) = halo(st, R), halo(st + 1, R)
            pl_c = pl_c + (alpha * a_lo + beta * b_lo)
            ph_c = ph_c + (alpha * a_hi + beta * b_hi)
            shift = h11
        else:
            ga = 1.0 - w1 * shift - w2 * zf
            gb = w1 + w2 * ze
            for i, v in enumerate((alpha, beta, ga, gb, w2)):
                fin[i:i + 1, :] = jnp.broadcast_to(v, (1, W))

    for st, part, n in sent:
        for to, _, c in copies(st, part, n):
            @pl.when(to)
            def _(c=c):
                c.wait_send()


def finish_kernel(L, NX, NY, pre, are, bre, cre, fin, p_out, l_out):
    alpha, beta, ga, gb, w2 = [fin[i:i + 1, 0:1] for i in range(5)]
    k = pl.program_id(0)

    def end(r, c):
        at = pl.ds(pl.multiple_of((r + 1) * T, T), T)
        here = pl.ds(pl.multiple_of(r * T, T), T)
        a, b = are[k, at, :], bre[k, at, :]
        p_out[0, here, :] = pre[k, at, :] + (alpha * a + beta * b)
        l_out[0, here, :] = ga * a - gb * b - w2 * cre[k, here, :]
        return c

    lax.fori_loop(0, NX // T, end, 0, unroll=True)


def body(pressure, pressure_old, conductivity, porosity, recharge, active):
    L, NX, NY = pressure.shape
    GX, GY = lax.axis_size("gx"), lax.axis_size("gy")
    f32 = jnp.float32
    cell = pltpu.VMEM((L, NX, NY), f32)
    ext = pltpu.VMEM((L, NX + 2 * T, NY), f32)
    ST = 1 + 2 * NEWTON
    NR0 = ((2 * L + 1 + T - 1) // T) * T
    dma = pltpu.SemaphoreType.DMA
    vm = pl.BlockSpec(memory_space=pltpu.VMEM)
    mid = pl.pallas_call(
        functools.partial(kernel, L, NX, NY, GX, GY),
        out_shape=(ext, ext, ext, cell, pltpu.VMEM((T, W), f32)),
        in_specs=[pl.BlockSpec(memory_space=pltpu.HBM)] * 6,
        out_specs=(vm,) * 5,
        scratch_shapes=[ext] + [pltpu.VMEM((1, NX + 2 * T, NY), f32), cell, cell]
        + [cell] * 5 + [cell] * 7
        + [
            pltpu.VMEM((ST, 2, NR0, NY), f32), pltpu.VMEM((ST, 2, 2, 3 * T, W), f32),
            pltpu.VMEM((ST, 2, NR0, NY), f32), pltpu.VMEM((ST, 2, 2, 3 * T, W), f32),
            pltpu.VMEM((NEWTON, GY, T, W), f32), pltpu.VMEM((NEWTON, GX, T, W), f32),
            pltpu.VMEM((NX, NY), jnp.int32), pltpu.VMEM((NX, NY), f32), dma((6,)),
            dma((ST, 3, 2)), dma((ST, 3, 2)),
            dma((NEWTON, GY)), dma((NEWTON, GY)), dma((NEWTON, GX)), dma((NEWTON, GX)),
        ],
        compiler_params=pltpu.CompilerParams(
            collective_id=0, has_side_effects=True, vmem_limit_bytes=60600000
        ),
    )(pressure, pressure_old, conductivity, porosity, recharge, active)
    block = pl.BlockSpec((1, NX, NY), lambda k: (k, 0, 0))
    return pl.pallas_call(
        functools.partial(finish_kernel, L, NX, NY),
        grid=(L,),
        out_shape=(jax.ShapeDtypeStruct(pressure.shape, f32),) * 2,
        in_specs=[vm] * 5,
        out_specs=(block, block),
        compiler_params=pltpu.CompilerParams(vmem_limit_bytes=8000000),
    )(*[pltpu.with_memory_space_constraint(m, pltpu.VMEM) for m in mid])


def solution(mesh):
    cells, flat = P(None, "gx", "gy"), P("gx", "gy")
    return jax.shard_map(
        body,
        mesh=mesh,
        in_specs=(cells, cells, cells, cells, flat, flat),
        out_specs=(cells, cells),
        check_vma=False,
    )
```

```python
import functools

import jax
import jax.numpy as jnp
from jax import lax
from jax.experimental import pallas as pl
from jax.experimental.pallas import tpu as pltpu
from jax.sharding import PartitionSpec as P

NEWTON = 2
residual_sat = 0.1
vertical_factor = 2.0
epsilon = 1e-06
T = 8
W = 128
MESH = pl.DeviceIdType.MESH


def sigmoid(v):
    return 1.0 / (1.0 + jnp.exp(jnp.minimum(-v, 87.0)))


def fold(v):
    out = v[:, :W]
    for j in range(1, v.shape[1] // W):
        out = out + v[:, j * W:(j + 1) * W]
    return out


def kernel(
    L, NX, NY, GX, GY,
    p_hbm, po_hbm, k_hbm, por_hbm, rech_hbm, act_hbm,
    pre, are, bre, cre, fin,
    sre, acte, p9, r0,
    txp, txm, typ, tym, tzp,
    dg, oxp, oxm, oyp, oym, ozp, ozm,
    srow, scol, rrow, rcol, sumy, sumx,
    act_in, rech_in, in_sem,
    send_sem, recv_sem, ysend, yrecv, xsend, xrecv,
):
    R = NX // T
    gx = lax.axis_index("gx")
    gy = lax.axis_index("gy")
    f32 = jnp.float32
    row8 = lax.broadcasted_iota(jnp.int32, (T, NY), 0)
    lane = lax.broadcasted_iota(jnp.int32, (T, NY), 1)
    lane1 = lax.broadcasted_iota(jnp.int32, (T, W), 1)
    has = (gx > 0, gx < GX - 1, gy > 0, gy < GY - 1)

    mid = pl.ds(T, NX)
    loads = [
        pltpu.make_async_copy(src, dst, in_sem.at[i])
        for i, (src, dst) in enumerate((
            (p_hbm, pre.at[:, mid, :]), (k_hbm, are.at[:, mid, :]), (act_hbm, act_in),
            (rech_hbm, rech_in), (por_hbm, p9), (po_hbm, r0),
        ))
    ]
    for c in loads:
        c.start()

    rrow[...] = jnp.zeros_like(rrow)
    rcol[...] = jnp.zeros_like(rcol)

    barrier = pltpu.get_barrier_semaphore()
    ALL = GX * GY <= 32
    if ALL:
        greet = [(gx * GY + gy + d) % (GX * GY) for d in range(1, GX * GY)]
        greet = [(o // GY, lax.rem(o, GY)) for o in greet]
    else:
        greet = [(lax.rem(gx + d, GX), gy) for d in range(1, GX)]
        greet += [(gx, lax.rem(gy + d, GY)) for d in range(1, GY)]
    for peer in greet:
        pl.semaphore_signal(barrier, inc=1, device_id=peer, device_id_type=MESH)

    def tile(ref, k, r):
        return ref[k, pl.ds(pl.multiple_of((r + 1) * T, T), T), :]

    def plain(ref, k, r):
        return ref[k, pl.ds(pl.multiple_of(r * T, T), T), :]

    def put(ref, k, r, v):
        ref[k, pl.ds(pl.multiple_of(r * T, T), T), :] = v

    def up(ref, k, r, cur):
        return pltpu.roll(jnp.where(row8 == T - 1, tile(ref, k, r - 1), cur), 1, 0)

    def down(ref, k, r, cur):
        return pltpu.roll(jnp.where(row8 == 0, tile(ref, k, r + 1), cur), T - 1, 0)

    def wide(v):
        return jnp.concatenate([v] * (NY // W), axis=1)

    def left(cur, halo, k, r):
        h = pltpu.roll(halo, lax.rem(W + 1 - (k * R + r), W), 1)
        return jnp.where(lane == 0, wide(h), pltpu.roll(cur, 1, 1))

    def right(cur, halo, k, r):
        h = pltpu.roll(halo, W - 1 - (k * R + r), 1)
        return jnp.where(lane == NY - 1, wide(h), pltpu.roll(cur, NY - 1, 1))

    def pack(acc, v, k, r):
        lo, hi = acc
        both = jnp.where(lane1 == 0, v[:, :W], v[:, NY - W:])
        both = pltpu.roll(both, k * R + r, 1)
        lo = jnp.where(lane1 == k * R + r, both, lo)
        hi = jnp.where(lane1 == lax.rem(k * R + r + W - 1, W), both, hi)
        return lo, hi

    zero1 = jnp.zeros((T, W), f32)

    peers = ((gx - 1, gy), (gx + 1, gy), (gx, gy - 1), (gx, gy + 1))

    def copies(st, part, n):
        out = []
        for d in (0, 1) if part == 0 else (2, 3):
            back = d ^ 1
            if part == 0:
                src, dst = srow.at[st, d, pl.ds(0, n)], rrow.at[st, back, pl.ds(0, n)]
            else:
                src = scol.at[st, part - 1, d - 2, pl.ds(0, n)]
                dst = rcol.at[st, part - 1, back - 2, pl.ds(0, n)]
            out.append((has[d], has[back], pltpu.make_async_remote_copy(
                src_ref=src, dst_ref=dst,
                send_sem=send_sem.at[st, part, d % 2], recv_sem=recv_sem.at[st, part, back % 2],
                device_id=peers[d], device_id_type=MESH)))
        return out

    def start(st, part, n):
        for to, _, c in copies(st, part, n):
            @pl.when(to)
            def _(c=c):
                c.start()

    sent = []

    def recv(st, part, n, also=True):
        sent.append((st, part, n))
        for _, frm, c in copies(st, part, n):
            @pl.when(jnp.logical_and(frm, also))
            def _(c=c):
                c.wait_recv()

    NR0 = srow.shape[2]
    NRL = ((L + T - 1) // T) * T

    for c in loads[:3]:
        c.wait()

    for e, row in ((0, 0), (1, NX - 1)):
        for k in range(L):
            srow[0, e, k:k + 1, :] = pre[k, T + row:T + row + 1, :]
            srow[0, e, L + k:L + k + 1, :] = are[k, T + row:T + row + 1, :]
        srow[0, e, 2 * L:2 * L + 1, :] = act_in[row:row + 1, :].astype(f32)

    def pack0(r, c):
        pp, kk, aa = c
        for k in range(L):
            pp = pack(pp, tile(pre, k, r), k, r)
            kk = pack(kk, tile(are, k, r), k, r)
        aa = pack(aa, act_in[pl.ds(pl.multiple_of(r * T, T), T), :].astype(f32), 0, r)
        return pp, kk, aa

    z2 = (zero1, zero1)
    pp, kk, aa = lax.fori_loop(0, R, pack0, (z2, z2, z2))
    for e in range(2):
        scol[0, 0, e, 0:T, :] = pp[e]
        scol[0, 0, e, T:2 * T, :] = kk[e]
        scol[0, 0, e, 2 * T:3 * T, :] = aa[e]
    pl.semaphore_wait(barrier, len(greet))
    start(0, 0, NR0)
    start(0, 1, 3 * T)
    for c in loads[3:]:
        c.wait()

    def local(r, c):
        act = act_in[pl.ds(pl.multiple_of(r * T, T), T), :].astype(f32)
        put(acte, 0, r + 1, act)
        for k in range(L):
            put(sre, k, r + 1, sigmoid(tile(pre, k, r)))
            w = (1.0 - residual_sat) * act * plain(p9, k, r)
            put(p9, k, r, w)
            base = w * sigmoid(plain(r0, k, r))
            if k == L - 1:
                base = base + act * rech_in[pl.ds(pl.multiple_of(r * T, T), T), :]
            put(r0, k, r, base)
        return c

    lax.fori_loop(0, R, local, 0)
    recv(0, 0, NR0)
    recv(0, 1, 3 * T)

    def halo_rows(ref, st, base):
        for e, row in ((0, T - 1), (1, T + NX)):
            for k in range(L):
                ref[k, row:row + 1, :] = rrow[st, e, base + k:base + k + 1, :]

    halo_rows(pre, 0, 0)
    halo_rows(are, 0, L)
    for e, row in ((0, T - 1), (1, T + NX)):
        acte[0, row:row + 1, :] = rrow[0, e, 2 * L:2 * L + 1, :]
        for k in range(L):
            sre[k, row:row + 1, :] = sigmoid(rrow[0, e, k:k + 1, :])

    kl, kh = rcol[0, 0, 0, T:2 * T, :], rcol[0, 0, 1, T:2 * T, :]
    al, ah = rcol[0, 0, 0, 2 * T:3 * T, :], rcol[0, 0, 1, 2 * T:3 * T, :]

    def trans(r, c):
        act = tile(acte, 0, r)
        ha = 0.5 * act
        a_up = ha * up(acte, 0, r, act)
        a_dn = ha * down(acte, 0, r, act)
        a_lf = ha * left(act, al, 0, r)
        a_rt = ha * right(act, ah, 0, r)
        av = vertical_factor * ha * act
        cur = tile(are, 0, r)
        for k in range(L):
            put(txm, k, r, a_up * (cur + up(are, k, r, cur)))
            put(txp, k, r, a_dn * (cur + down(are, k, r, cur)))
            put(tym, k, r, a_lf * (cur + left(cur, kl, k, r)))
            put(typ, k, r, a_rt * (cur + right(cur, kh, k, r)))
            if k < L - 1:
                nxt = tile(are, k + 1, r)
                put(tzp, k, r, av * (cur + nxt))
                cur = nxt
        return c

    lax.fori_loop(0, R, trans, 0)

    pl_c, ph_c = rcol[0, 0, 0, 0:T, :], rcol[0, 0, 1, 0:T, :]
    shift = jnp.zeros((1, 1), f32)
    H = max(2, R - 3)

    def order(i):
        return jnp.where(i < 2, i * (R - 1), i - 1)

    def emit(ref, st, i, acc):
        @pl.when(i == 1)
        def _():
            for e, row in ((0, T), (1, T + NX - 1)):
                for k in range(L):
                    srow[st, e, k:k + 1, :] = ref[k, row:row + 1, :]
            start(st, 0, NRL)

        for part, at in ((1, H - 1), (2, R - 1)):
            @pl.when(i == at)
            def _(part=part):
                scol[st, part - 1, 0, 0:T, :] = acc[0]
                scol[st, part - 1, 1, 0:T, :] = acc[1]
                start(st, part, T)

    def ready(st, i):
        recv(st, 2, T, i == H)

    def halo(st, i):
        late = jnp.where(i < H, 0, 1)
        return rcol[st, late, 0, 0:T, :], rcol[st, late, 1, 0:T, :]

    for it in range(NEWTON):
        sl_c, sh_c = sigmoid(pl_c), sigmoid(ph_c)

        st = 1 + 2 * it

        def coef(i, acc):
            r = order(i)
            pc, sc = tile(pre, 0, r), tile(sre, 0, r)
            sm = sd = fl = None
            for k in range(L):
                s2 = sc * sc
                mc = 0.5 * s2
                s1 = 1.0 - sc
                ec = s2 * s1
                for pn, sn, tr, off in (
                    (up(pre, k, r, pc), up(sre, k, r, sc), txm, oxm),
                    (down(pre, k, r, pc), down(sre, k, r, sc), txp, oxp),
                    (left(pc, pl_c, k, r), left(sc, sl_c, k, r), tym, oym),
                    (right(pc, ph_c, k, r), right(sc, sh_c, k, r), typ, oyp),
                ):
                    n2 = sn * sn
                    t = plain(tr, k, r)
                    drop = pc - pn
                    tm = t * (mc + 0.5 * n2)
                    td = t * drop
                    put(off, k, r, n2 * (1.0 - sn) * td - tm)
                    if sm is None:
                        sm, sd, fl = tm, td, tm * drop
                    else:
                        sm, sd, fl = sm + tm, sd + td, fl + tm * drop
                if k < L - 1:
                    pn, sn = tile(pre, k + 1, r), tile(sre, k + 1, r)
                    n2 = sn * sn
                    t = plain(tzp, k, r)
                    drop = pc - pn - 1.0
                    tm = t * (mc + 0.5 * n2)
                    td = t * drop
                    f = tm * drop
                    put(ozp, k, r, n2 * (1.0 - sn) * td - tm)
                    put(ozm, k + 1, r, -(ec * td + tm))
                    sm, sd, fl = sm + tm, sd + td, fl + f
                w = plain(p9, k, r)
                rest = 1.0 - tile(acte, 0, r)
                put(dg, k, r, w * sc * s1 + rest + sm + ec * sd)
                q = plain(r0, k, r) - w * sc - fl - rest * pc
                put(are, k, r + 1, q)
                acc = pack(acc, q, k, r)
                if k < L - 1:
                    pc, sc = pn, sn
                    sm, sd, fl = tm, -td, -f
            emit(are, st, i, acc)
            return acc

        def apply(ref, k, r, cur, before, after, lo, hi):
            y = plain(dg, k, r) * cur
            y = y + plain(oxm, k, r) * up(ref, k, r, cur)
            y = y + plain(oxp, k, r) * down(ref, k, r, cur)
            y = y + plain(oym, k, r) * left(cur, lo, k, r)
            y = y + plain(oyp, k, r) * right(cur, hi, k, r)
            if before is not None:
                y = y + plain(ozm, k, r) * before
            if after is not None:
                y = y + plain(ozp, k, r) * after
            return y - shift * cur

        lax.fori_loop(0, R, coef, z2)
        recv(st, 0, NRL)
        recv(st, 1, T)
        halo_rows(are, st, 0)

        def first(i, c):
            r = order(i)
            ready(st, i)
            a_lo, a_hi = halo(st, i)
            acc, aa, ab, bb = c
            before, cur = None, tile(are, 0, r)
            for k in range(L):
                after = tile(are, k + 1, r) if k < L - 1 else None
                b = apply(are, k, r, cur, before, after, a_lo, a_hi)
                put(bre, k, r + 1, b)
                acc = pack(acc, b, k, r)
                aa = aa + fold(cur * cur)
                ab = ab + fold(cur * b)
                bb = bb + fold(b * b)
                before, cur = cur, after
            emit(bre, st + 1, i, acc)
            return acc, aa, ab, bb

        acc, aa, ab, bb = lax.fori_loop(0, R, first, (z2, zero1, zero1, zero1))
        recv(st + 1, 0, NRL)
        recv(st + 1, 1, T)
        halo_rows(bre, st + 1, 0)
        last = it == NEWTON - 1

        def second(i, c):
            r = order(i)
            ready(st + 1, i)
            b_lo, b_hi = halo(st + 1, i)
            ac, bc, cc = c
            before, cur = None, tile(bre, 0, r)
            for k in range(L):
                after = tile(bre, k + 1, r) if k < L - 1 else None
                v = apply(bre, k, r, cur, before, after, b_lo, b_hi)
                if last:
                    put(cre, k, r, v)
                ac = ac + fold(tile(are, k, r) * v)
                bc = bc + fold(cur * v)
                cc = cc + fold(v * v)
                before, cur = cur, after
            return ac, bc, cc

        ac, bc, cc = lax.fori_loop(0, R, second, (zero1, zero1, zero1))

        for i, v in enumerate((aa, ab, bb, ac, bc, cc)):
            sumy[it, 0, i:i + 1, :] = jnp.sum(v, axis=0, keepdims=True)
        for i in range(6, T):
            sumy[it, 0, i:i + 1, :] = jnp.zeros((1, W), f32)

        def spread(buf, n, mine, device, ss, rs):
            cps = []
            for d in range(1, n):
                c = pltpu.make_async_remote_copy(
                    src_ref=buf.at[it, 0], dst_ref=buf.at[it, d],
                    send_sem=ss.at[it, d], recv_sem=rs.at[it, d],
                    device_id=device(lax.rem(mine + d, n)), device_id_type=MESH)
                c.start()
                cps.append(c)
            for c in cps:
                c.wait()
            tot = buf[it, 0]
            for d in range(1, n):
                tot = tot + buf[it, d]
            return tot

        def flat(o):
            return (o // GY, lax.rem(o, GY))

        if ALL:
            tot = spread(sumy, GX * GY, gx * GY + gy, flat, ysend, yrecv)
        else:
            tot = spread(sumy, GY, gy, lambda o: (gx, o), ysend, yrecv)
            sumx[it, 0] = tot
            tot = spread(sumx, GX, gx, lambda o: (o, gy), xsend, xrecv)
        g = jnp.sum(tot, axis=1, keepdims=True)
        aa, ab, bb, ac, bc, cc = [g[i:i + 1, :] for i in range(6)]

        n2 = aa + epsilon
        n0 = jnp.sqrt(n2)
        dl = (ab - shift * epsilon) / n2
        h11 = shift + dl
        uu = jnp.maximum(bb - 2.0 * dl * ab + dl * dl * aa, 0.0) / n2
        h21s = uu + epsilon
        h21 = jnp.sqrt(h21s)
        ze = shift - dl
        zf = -dl * shift
        za = ac + ze * ab + zf * aa
        zb = bc + ze * bb + zf * ab
        zc = cc + ze * bc + zf * ac
        sc2 = n2 * h21s
        h12 = za / (n2 * h21)
        h22 = (zb - dl * za) / sc2
        zz = (zc + ze * zb + zf * za) / sc2
        v11 = aa / n2
        v22 = uu / h21s
        v12 = h11 * epsilon / (n2 * h21)
        u2 = zz - (2.0 - v11) * h12 * h12 - (2.0 - v22) * h22 * h22 + 2.0 * h12 * h22 * v12
        h32s = jnp.maximum(u2, 0.0) + epsilon
        r1 = jnp.sqrt(h11 * h11 + h21s)
        co, si = h11 / r1, h21 / r1
        tr = co * h12 + si * h22
        lo = co * h22 - si * h12
        y2 = -lo * si * n0 / (lo * lo + h32s)
        y1 = (co * n0 - tr * y2) / r1
        w1 = y1 / n0
        w2 = y2 / (n0 * h21)
        alpha, beta = w1 - w2 * dl, w2

        if not last:
            def step(r, c):
                for k in range(L):
                    p = plain(pre, k, r) + (alpha * plain(are, k, r) + beta * plain(bre, k, r))
                    put(pre, k, r, p)
                    put(sre, k, r, sigmoid(p))
                return c

            lax.fori_loop(0, R + 2, step, 0)
            (a_lo, a_hi), (b_lo, b_hi) = halo(st, R), halo(st + 1, R)
            pl_c = pl_c + (alpha * a_lo + beta * b_lo)
            ph_c = ph_c + (alpha * a_hi + beta * b_hi)
            shift = h11
        else:
            ga = 1.0 - w1 * shift - w2 * zf
            gb = w1 + w2 * ze
            for i, v in enumerate((alpha, beta, ga, gb, w2)):
                fin[i:i + 1, :] = jnp.broadcast_to(v, (1, W))

    for st, part, n in sent:
        for to, _, c in copies(st, part, n):
            @pl.when(to)
            def _(c=c):
                c.wait_send()


def finish_kernel(L, NX, NY, pre, are, bre, cre, fin, p_out, l_out):
    alpha, beta, ga, gb, w2 = [fin[i:i + 1, 0:1] for i in range(5)]
    k = pl.program_id(0)

    def end(r, c):
        at = pl.ds(pl.multiple_of((r + 1) * T, T), T)
        here = pl.ds(pl.multiple_of(r * T, T), T)
        a, b = are[k, at, :], bre[k, at, :]
        p_out[0, here, :] = pre[k, at, :] + (alpha * a + beta * b)
        l_out[0, here, :] = ga * a - gb * b - w2 * cre[k, here, :]
        return c

    lax.fori_loop(0, NX // T, end, 0, unroll=True)


def body(pressure, pressure_old, conductivity, porosity, recharge, active):
    L, NX, NY = pressure.shape
    GX, GY = lax.axis_size("gx"), lax.axis_size("gy")
    f32 = jnp.float32
    cell = pltpu.VMEM((L, NX, NY), f32)
    ext = pltpu.VMEM((L, NX + 2 * T, NY), f32)
    ST = 1 + 2 * NEWTON
    SY = GX * GY if GX * GY <= 32 else GY
    NR0 = ((2 * L + 1 + T - 1) // T) * T
    dma = pltpu.SemaphoreType.DMA
    vm = pl.BlockSpec(memory_space=pltpu.VMEM)
    mid = pl.pallas_call(
        functools.partial(kernel, L, NX, NY, GX, GY),
        out_shape=(ext, ext, ext, cell, pltpu.VMEM((T, W), f32)),
        in_specs=[pl.BlockSpec(memory_space=pltpu.HBM)] * 6,
        out_specs=(vm,) * 5,
        scratch_shapes=[ext] + [pltpu.VMEM((1, NX + 2 * T, NY), f32), cell, cell]
        + [cell] * 5 + [cell] * 7
        + [
            pltpu.VMEM((ST, 2, NR0, NY), f32), pltpu.VMEM((ST, 2, 2, 3 * T, W), f32),
            pltpu.VMEM((ST, 2, NR0, NY), f32), pltpu.VMEM((ST, 2, 2, 3 * T, W), f32),
            pltpu.VMEM((NEWTON, SY, T, W), f32), pltpu.VMEM((NEWTON, GX, T, W), f32),
            pltpu.VMEM((NX, NY), jnp.int32), pltpu.VMEM((NX, NY), f32), dma((6,)),
            dma((ST, 3, 2)), dma((ST, 3, 2)),
            dma((NEWTON, SY)), dma((NEWTON, SY)), dma((NEWTON, GX)), dma((NEWTON, GX)),
        ],
        compiler_params=pltpu.CompilerParams(
            collective_id=0, has_side_effects=True, vmem_limit_bytes=60600000
        ),
    )(pressure, pressure_old, conductivity, porosity, recharge, active)
    block = pl.BlockSpec((1, NX, NY), lambda k: (k, 0, 0))
    return pl.pallas_call(
        functools.partial(finish_kernel, L, NX, NY),
        grid=(L,),
        out_shape=(jax.ShapeDtypeStruct(pressure.shape, f32),) * 2,
        in_specs=[vm] * 5,
        out_specs=(block, block),
        compiler_params=pltpu.CompilerParams(vmem_limit_bytes=8000000),
    )(*[pltpu.with_memory_space_constraint(m, pltpu.VMEM) for m in mid])


def solution(mesh):
    cells, flat = P(None, "gx", "gy"), P("gx", "gy")
    return jax.shard_map(
        body,
        mesh=mesh,
        in_specs=(cells, cells, cells, cells, flat, flat),
        out_specs=(cells, cells),
        check_vma=False,
    )
```
